128 devices in a mesh: south: 2 (over x_hi), east: 8 (over y, core), down: 8 (over z, x_lo).
Axes of the slice: x: 4 (x_hi: 2, x_lo: 2; x = x_hi * 2 + x_lo), y: 4, z: 4, core: 2. Of those that a mesh axis runs over, the one named last changes fastest.
Arguments:
- field_values: float32 [256, 64, 64, 128], P('south', 'east', 'down'), may hold values from 0.5 to 2
- flow_j: float32 [256, 64, 64, 128], P('south', 'east', 'down'), may hold values from -0.3 to 0.3
- flow_i: float32 [256, 64, 64, 128], P('south', 'east', 'down'), may hold values from -0.3 to 0.3
- flow_k: float32 [256, 64, 64, 128], P('south', 'east', 'down'), may hold values from -0.3 to 0.3
Outputs:
- standardized: float32 [256, 64, 64, 128], P('south', 'east', 'down')
- field_values_end: float32 [256, 64, 64, 128], P('south', 'east', 'down')
The draws below stay inside these ranges and needn't reach their ends.
All inputs are finite; a program needn't handle non-finite values.
Results may differ from the reference program's by a relative error of at most 0.00002.
Values sent between devices are 32-bit elements; how exact they have to be, the bound alone decides.
No kernel may reach another device: no remote copies, remote signals or barrier semaphores. Data moves between devices by JAX's collectives and lax.ppermute only.
A program may use at most 128 MiB of HBM per device.

```python
import jax
import jax.numpy as jnp
from jax import lax

GRID_J = 256
GRID_I = 64
GRID_K = 64
LEVELS = 128
STEPS = 6


def block_scale(key, shape, cuts, smallest, high):
    def one(dim, blocks):
        steps = jax.random.uniform(jax.random.fold_in(jax.random.fold_in(key, 6), dim), (blocks,), jnp.float32, smallest / len(cuts), high / len(cuts))
        return jnp.repeat(jnp.exp(steps), shape[dim] // blocks).reshape((-1,) + (1,) * (len(shape) - dim - 1))

    level = one(*cuts[0])
    for cut in cuts[1:]:
        level = level * one(*cut)
    return level


def setup_inputs(seed: int = 0) -> dict:
    key_of = jax.random.split(jax.random.key(seed), 5)
    return {
        "field_values": jnp.clip(0.5 + 1.5 * jax.random.uniform(key_of[0], (GRID_J, GRID_I, GRID_K, LEVELS), jnp.float32) ** block_scale(key_of[0], (GRID_J, GRID_I, GRID_K, LEVELS), ((0, 2), (1, 8), (2, 8)), -0.2, 0.2), 0.5, 2.0),
        "flow_j": jnp.clip(jax.random.uniform(key_of[1], (GRID_J, GRID_I, GRID_K, LEVELS), jnp.float32, -0.3, 0.3) * block_scale(key_of[1], (GRID_J, GRID_I, GRID_K, LEVELS), ((0, 2), (1, 8), (2, 8)), -0.4, 0.0), -0.3, 0.3),
        "flow_i": jnp.clip(jax.random.uniform(key_of[2], (GRID_J, GRID_I, GRID_K, LEVELS), jnp.float32, -0.3, 0.3) * block_scale(key_of[2], (GRID_J, GRID_I, GRID_K, LEVELS), ((0, 2), (1, 8), (2, 8)), -0.4, 0.0), -0.3, 0.3),
        "flow_k": jnp.clip(jax.random.uniform(key_of[3], (GRID_J, GRID_I, GRID_K, LEVELS), jnp.float32, -0.3, 0.3) * block_scale(key_of[3], (GRID_J, GRID_I, GRID_K, LEVELS), ((0, 2), (1, 8), (2, 8)), -0.4, 0.0), -0.3, 0.3),
    }


def inner_cells(values, dims):
    for dim in dims:
        values = lax.slice_in_dim(values, 1, values.shape[dim] - 1, axis=dim)
    return values

def side_cells(values, dim, start, dims):
    others = [other for other in dims if other != dim]
    values = inner_cells(values, others)
    return lax.slice_in_dim(values, start, start + values.shape[dim] - 2, axis=dim)

def advance(padded, flow_j, flow_i, flow_k):
    middle = inner_cells(padded, (0, 1, 2))
    lower = [side_cells(padded, dim, 0, (0, 1, 2)) for dim in (0, 1, 2)]
    upper = [side_cells(padded, dim, 2, (0, 1, 2)) for dim in (0, 1, 2)]
    slopes = [above - below for above, below in zip(upper, lower)]
    smooth_rate = 0.05
    spread = lower[0] + upper[0] + lower[1] + upper[1] + lower[2] + upper[2] - 6.0 * middle
    return middle - flow_j * slopes[0] - flow_i * slopes[1] - flow_k * slopes[2] + smooth_rate * spread

def reference(field_values, flow_j, flow_i, flow_k):
    for step in range(STEPS):
        field_values = advance(jnp.pad(field_values, ((1, 1), (1, 1), (1, 1), (0, 0)), mode='constant'), flow_j, flow_i, flow_k)
    line_mean = lax.optimization_barrier(jnp.mean(field_values, axis=0, keepdims=True))
    centred = field_values - line_mean
    line_variance = lax.optimization_barrier(jnp.mean(centred * centred, axis=0, keepdims=True))
    standardized = centred * lax.rsqrt(line_variance + 0.0001)
    return (standardized, field_values)
```

```python
import jax
import jax.numpy as jnp
from jax import lax
from jax.experimental import pallas as pl
from jax.experimental.pallas import tpu as pltpu
from jax.sharding import PartitionSpec as P


STEPS = 6
RATE = 0.05
F32 = jnp.float32
VMEM = pltpu.VMEM
SMEM = pltpu.SMEM


def swap_pairs(devices, first):
    pairs = []
    for a in range(first, devices - 1, 2):
        pairs += [(a, a + 1), (a + 1, a)]
    return pairs


def combine(c, jl, ju, il, iu, kl, ku, fj, fi, fk):
    total = (jl + ju) + (il + iu) + (kl + ku)
    return (
        c * (1.0 - 6.0 * RATE)
        + RATE * total
        - fj * (ju - jl)
        - fi * (iu - il)
        - fk * (ku - kl)
    )


def face_body(side, flags, f, fj, fi, fk, halo, e1, e2, s, out):
    rows, ni, nl = out.shape
    nk = f.shape[1] // ni
    last = flags[0] == side
    k = jnp.where(last, nk - 1, 0)
    kin = jnp.where(last, nk - 2, 1)
    sign = jnp.where(last, F32(1), F32(-1))
    i_even = flags[1] == 0
    low_south = flags[2] == 0
    sub = lax.broadcasted_iota(jnp.int32, (ni, nl), 0)
    e1_edge = sub == jnp.where(i_even, ni - 1, 0)
    first_i = sub == 0
    last_i = sub == ni - 1

    def at(ref, j, kk):
        return ref[j, pl.ds(kk, ni, stride=nk), :]

    beyond = s[pl.ds(k, ni, stride=nk), :]
    zero = jnp.zeros_like(beyond)

    def row(j, prev, cur, nxt):
        r1 = jnp.broadcast_to(e1[j, pl.ds(k, 1), :], (ni, nl))
        r2 = jnp.broadcast_to(e2[j, pl.ds(k, 1), :], (ni, nl))
        edge = jnp.where(e1_edge, r1, r2)
        il = jnp.where(first_i, edge, pltpu.roll(cur, 1, 0))
        iu = jnp.where(last_i, edge, pltpu.roll(cur, ni - 1, 0))
        h = halo[j]
        inner = at(f, j, kin)
        out[j] = combine(
            cur, prev, nxt, il, iu, inner, h,
            at(fj, j, k), at(fi, j, k), sign * at(fk, j, k),
        )

    def body(j, carry):
        prev, cur = carry
        nxt = at(f, j + 1, k)
        row(j, prev, cur, nxt)
        return cur, nxt

    prev, cur = lax.fori_loop(
        0, rows - 1, body, (jnp.where(low_south, zero, beyond), at(f, 0, k)), unroll=False
    )
    row(rows - 1, prev, cur, jnp.where(low_south, beyond, zero))


def update_rows(flags, f, fj, fi, fk, ha, hb, e1, e2, s, emit):
    rows, ni, nk, nl = f.shape
    i_even = flags[1] == 0
    low_south = flags[2] == 0
    sub = lax.broadcasted_iota(jnp.int32, (nk, nl), 0)
    a_edge = sub == jnp.where(flags[0] == 0, nk - 1, 0)
    first_k = sub == 0
    last_k = sub == nk - 1

    def row(j, prev, cur, nxt):
        x1 = e1[j]
        x2 = e2[j]
        below = jnp.where(i_even, x2, x1)
        above = jnp.where(i_even, x1, x2)
        new = []
        for i in range(ni):
            c = cur[i]
            ra = jnp.broadcast_to(ha[j, pl.ds(i, 1), :], (nk, nl))
            rb = jnp.broadcast_to(hb[j, pl.ds(i, 1), :], (nk, nl))
            edge = jnp.where(a_edge, ra, rb)
            kl = jnp.where(first_k, edge, pltpu.roll(c, 1, 0))
            ku = jnp.where(last_k, edge, pltpu.roll(c, nk - 1, 0))
            il = below if i == 0 else cur[i - 1]
            iu = above if i == ni - 1 else cur[i + 1]
            new.append(
                combine(c, prev[i], nxt[i], il, iu, kl, ku, fj[j, i], fi[j, i], fk[j, i])
            )
        emit(j, new)

    def body(j, carry):
        prev, cur = carry
        nxt = tuple(f[j + 1, i] for i in range(ni))
        row(j, prev, cur, nxt)
        return cur, nxt

    zero = jnp.zeros((nk, nl), F32)
    start = (
        tuple(jnp.where(low_south, zero, s[i]) for i in range(ni)),
        tuple(f[0, i] for i in range(ni)),
    )
    prev, cur = lax.fori_loop(0, rows - 1, body, start, unroll=False)
    row(rows - 1, prev, cur, tuple(jnp.where(low_south, s[i], zero) for i in range(ni)))


def full_body(flags, f, fj, fi, fk, ha, hb, e1, e2, s, order, out, g1, g2, gs):
    rows, ni, _, _ = f.shape
    i_even = flags[1] == 0

    def emit(j, new):
        for i in range(ni):
            out[j, i] = new[i]
        g1[j] = jnp.where(i_even, new[-1], new[0])
        g2[j] = jnp.where(i_even, new[0], new[-1])

    update_rows(flags, f, fj, fi, fk, ha, hb, e1, e2, s, emit)
    gs[...] = out[jnp.where(flags[2] == 0, rows - 1, 0)]


def final_body(flags, f, fj, fi, fk, ha, hb, e1, e2, s, out, stats):
    rows, ni, nk, nl = f.shape

    def emit(j, new):
        for i in range(ni):
            out[j, i] = new[i]

    update_rows(flags, f, fj, fi, fk, ha, hb, e1, e2, s, emit)
    zero = tuple(jnp.zeros((nk, nl), F32) for _ in range(ni))

    def add(j, sums):
        return tuple(a + out[j, i] for i, a in enumerate(sums))

    means = tuple(a * (1.0 / rows) for a in lax.fori_loop(0, rows, add, zero, unroll=2))

    def add_square(j, sums):
        new = []
        for i, a in enumerate(sums):
            d = out[j, i] - means[i]
            new.append(a + d * d)
        return tuple(new)

    spread = lax.fori_loop(0, rows, add_square, zero, unroll=2)
    for i in range(ni):
        stats[0, i] = means[i]
        stats[1, i] = spread[i]


def scale_body(f, mine, other, out):
    rows, ni, _, _ = f.shape
    mean = []
    scale = []
    for i in range(ni):
        apart = mine[0, i] - other[0, i]
        mean.append(0.5 * (mine[0, i] + other[0, i]))
        squares = mine[1, i] + other[1, i] + (0.5 * rows) * (apart * apart)
        scale.append(lax.rsqrt(squares * (0.5 / rows) + 0.0001))

    def body(j, _):
        for i in range(ni):
            out[j, i] = (f[j, i] - mean[i]) * scale[i]
        return 0

    lax.fori_loop(0, rows, body, 0, unroll=2)


def edges_body(flags, f, g1, g2, ga, gb, gs):
    rows, ni, nk, _ = f.shape
    i_even = flags[1] == 0
    a_last = flags[0] == 0

    def body(j, _):
        g1[j] = jnp.where(i_even, f[j, ni - 1], f[j, 0])
        g2[j] = jnp.where(i_even, f[j, 0], f[j, ni - 1])
        lo = f[j, :, 0, :]
        hi = f[j, :, nk - 1, :]
        ga[j] = jnp.where(a_last, hi, lo)
        gb[j] = jnp.where(a_last, lo, hi)
        return 0

    lax.fori_loop(0, rows, body, 0)
    gs[...] = f[jnp.where(flags[2] == 0, rows - 1, 0)]


def call(body, args, outs, mib=2):
    flagged = args[0].dtype == jnp.int32
    specs = [pl.BlockSpec(memory_space=VMEM) for _ in args]
    if flagged:
        specs[0] = pl.BlockSpec(memory_space=SMEM)
    return pl.pallas_call(
        body,
        out_shape=[jax.ShapeDtypeStruct(o, F32) for o in outs],
        in_specs=specs,
        out_specs=[pl.BlockSpec(memory_space=VMEM) for _ in outs],
        compiler_params=pltpu.CompilerParams(vmem_limit_bytes=mib << 20),
    )(*args)


def per_device(field, fj, fi, fk):
    import functools

    rows, ni, nk, nl = field.shape
    flags = jnp.stack(
        [
            lax.axis_index("down") % 2,
            lax.axis_index("east") % 2,
            lax.axis_index("south"),
        ]
    ).astype(jnp.int32)

    def swap(x, axis, first):
        return lax.ppermute(x, axis, swap_pairs(lax.axis_size(axis), first))

    flat = (rows, ni * nk, nl)
    kface, iface, jface = (rows, ni, nl), (rows, nk, nl), (ni, nk, nl)
    fjr, fir, fkr = (x.reshape(flat) for x in (fj, fi, fk))

    g1, g2, ga, gb, gs = call(edges_body, [flags, field], [iface, iface, kface, kface, jface])
    ha = swap(ga, "down", 0)
    hb = swap(gb, "down", 1)
    e2 = swap(g2, "east", 1)
    e1 = swap(g1, "east", 0)
    s = swap(gs, "south", 0)
    for _ in range(STEPS - 1):
        fr = field.reshape(flat)
        sr = s.reshape(ni * nk, nl)
        (ga,) = call(functools.partial(face_body, 0), [flags, fr, fjr, fir, fkr, ha, e1, e2, sr], [kface])
        (gb,) = call(functools.partial(face_body, 1), [flags, fr, fjr, fir, fkr, hb, e1, e2, sr], [kface])
        ha_next = swap(ga, "down", 0)
        hb_next = swap(gb, "down", 1)
        field, g1, g2, gs = call(
            full_body, [flags, field, fj, fi, fk, ha, hb, e1, e2, s, gb],
            [field.shape, iface, iface, jface],
        )
        ha, hb = ha_next, hb_next
        e2 = swap(g2, "east", 1)
        e1 = swap(g1, "east", 0)
        s = swap(gs, "south", 0)
    field, stats = call(
        final_body, [flags, field, fj, fi, fk, ha, hb, e1, e2, s],
        [field.shape, (2, ni, nk, nl)], 12,
    )
    other = swap(stats, "south", 0)
    (standardized,) = call(scale_body, [field, stats, other], [field.shape], 12)
    return (standardized, field)


def solution(mesh):
    spec = P("south", "east", "down", None)
    return jax.shard_map(
        per_device,
        mesh=mesh,
        in_specs=(spec,) * 4,
        out_specs=(spec, spec),
        check_vma=False,
    )
```

```python
import jax
import jax.numpy as jnp
from jax import lax
from jax.experimental import pallas as pl
from jax.experimental.pallas import tpu as pltpu
from jax.sharding import PartitionSpec as P


STEPS = 6
RATE = 0.05
F32 = jnp.float32
VMEM = pltpu.VMEM
SMEM = pltpu.SMEM
HBM = pltpu.HBM
ROWS = 8


def swap_pairs(devices, first):
    pairs = []
    for a in range(first, devices - 1, 2):
        pairs += [(a, a + 1), (a + 1, a)]
    return pairs


def combine(c, jl, ju, il, iu, kl, ku, fj, fi, fk):
    total = (jl + ju) + (il + iu) + (kl + ku)
    return (
        c * (1.0 - 6.0 * RATE)
        + RATE * total
        - fj * (ju - jl)
        - fi * (iu - il)
        - fk * (ku - kl)
    )


def face_body(side, flags, f, fj, fi, fk, halo, e1, e2, s, out):
    rows, ni, nl = out.shape
    nk = f.shape[1] // ni
    last = flags[0] == side
    k = jnp.where(last, nk - 1, 0)
    kin = jnp.where(last, nk - 2, 1)
    sign = jnp.where(last, F32(1), F32(-1))
    i_even = flags[1] == 0
    low_south = flags[2] == 0
    sub = lax.broadcasted_iota(jnp.int32, (ni, nl), 0)
    e1_edge = sub == jnp.where(i_even, ni - 1, 0)
    first_i = sub == 0
    last_i = sub == ni - 1

    def at(ref, j, kk):
        return ref[j, pl.ds(kk, ni, stride=nk), :]

    beyond = s[pl.ds(k, ni, stride=nk), :]
    zero = jnp.zeros_like(beyond)
    before = jnp.where(low_south, zero, beyond)
    after = jnp.where(low_south, beyond, zero)

    def body(t, prev):
        j0 = t * ROWS
        cur = [at(f, j0 + r, k) for r in range(ROWS)]
        nxt = jnp.where(j0 + ROWS == rows, after, at(f, jnp.minimum(j0 + ROWS, rows - 1), k))
        for r in range(ROWS):
            j, c = j0 + r, cur[r]
            r1 = jnp.broadcast_to(e1[j, pl.ds(k, 1), :], (ni, nl))
            r2 = jnp.broadcast_to(e2[j, pl.ds(k, 1), :], (ni, nl))
            edge = jnp.where(e1_edge, r1, r2)
            il = jnp.where(first_i, edge, pltpu.roll(c, 1, 0))
            iu = jnp.where(last_i, edge, pltpu.roll(c, ni - 1, 0))
            out[j] = combine(
                c, cur[r - 1] if r else prev, cur[r + 1] if r + 1 < ROWS else nxt,
                il, iu, at(f, j, kin), halo[j],
                at(fj, j, k), at(fi, j, k), sign * at(fk, j, k),
            )
        return cur[-1]

    lax.fori_loop(0, rows // ROWS, body, before)


def edge_body(flags, f, fj, fi, fk, ha, hb, e1, e2, s, order, g1, g2, gs):
    rows, ni, nk, nl = f.shape
    i_even = flags[1] == 0
    low_south = flags[2] == 0
    sub = lax.broadcasted_iota(jnp.int32, (nk, nl), 0)
    a_edge = sub == jnp.where(flags[0] == 0, nk - 1, 0)
    first_k = sub == 0
    last_k = sub == nk - 1
    zero = jnp.zeros((nk, nl), F32)

    def cell(j, i, c, prev, nxt, il, iu):
        ra = jnp.broadcast_to(ha[j, pl.ds(i, 1), :], (nk, nl))
        rb = jnp.broadcast_to(hb[j, pl.ds(i, 1), :], (nk, nl))
        edge = jnp.where(a_edge, ra, rb)
        kl = jnp.where(first_k, edge, pltpu.roll(c, 1, 0))
        ku = jnp.where(last_k, edge, pltpu.roll(c, nk - 1, 0))
        return combine(c, prev, nxt, il, iu, kl, ku, fj[j, i], fi[j, i], fk[j, i])

    def sides(j):
        x1, x2 = e1[j], e2[j]
        return jnp.where(i_even, x2, x1), jnp.where(i_even, x1, x2)

    js = jnp.where(low_south, rows - 1, 0)
    jin = jnp.where(low_south, rows - 2, 1)
    below, above = sides(js)
    row = [f[js, i] for i in range(ni)]
    for i in range(ni):
        inner = f[jin, i]
        gs[i] = cell(
            js, i, row[i], jnp.where(low_south, inner, s[i]), jnp.where(low_south, s[i], inner),
            row[i - 1] if i else below, row[i + 1] if i + 1 < ni else above,
        )

    before = tuple(jnp.where(low_south, zero, s[i]) for i in (0, ni - 1))
    after = tuple(jnp.where(low_south, s[i], zero) for i in (0, ni - 1))
    n = ROWS // 2

    def body(t, prev):
        j0 = t * n
        end = j0 + n == rows
        jn = jnp.minimum(j0 + n, rows - 1)
        cur = [(f[j0 + r, 0], f[j0 + r, ni - 1]) for r in range(n)]
        cur.append(tuple(jnp.where(end, a, f[jn, i]) for a, i in zip(after, (0, ni - 1))))
        cur.insert(0, prev)
        for r in range(n):
            j = j0 + r
            below, above = sides(j)
            lo = cell(j, 0, cur[r + 1][0], cur[r][0], cur[r + 2][0], below, f[j, 1])
            hi = cell(j, ni - 1, cur[r + 1][1], cur[r][1], cur[r + 2][1], f[j, ni - 2], above)
            g1[j] = jnp.where(i_even, hi, lo)
            g2[j] = jnp.where(i_even, lo, hi)
        return cur[n]

    lax.fori_loop(0, rows // n, body, before)


def update_rows(flags, f, fj, fi, fk, ha, hb, e1, e2, s, emit):
    rows, ni, nk, nl = f.shape
    i_even = flags[1] == 0
    low_south = flags[2] == 0
    sub = lax.broadcasted_iota(jnp.int32, (nk, nl), 0)
    a_edge = sub == jnp.where(flags[0] == 0, nk - 1, 0)
    first_k = sub == 0
    last_k = sub == nk - 1

    def row(j, prev, cur, nxt):
        x1 = e1[j]
        x2 = e2[j]
        below = jnp.where(i_even, x2, x1)
        above = jnp.where(i_even, x1, x2)
        new = []
        for i in range(ni):
            c = cur[i]
            ra = jnp.broadcast_to(ha[j, pl.ds(i, 1), :], (nk, nl))
            rb = jnp.broadcast_to(hb[j, pl.ds(i, 1), :], (nk, nl))
            edge = jnp.where(a_edge, ra, rb)
            kl = jnp.where(first_k, edge, pltpu.roll(c, 1, 0))
            ku = jnp.where(last_k, edge, pltpu.roll(c, nk - 1, 0))
            il = below if i == 0 else cur[i - 1]
            iu = above if i == ni - 1 else cur[i + 1]
            new.append(
                combine(c, prev[i], nxt[i], il, iu, kl, ku, fj[j, i], fi[j, i], fk[j, i])
            )
        emit(j, new)

    def body(j, carry):
        prev, cur = carry
        nxt = tuple(f[j + 1, i] for i in range(ni))
        row(j, prev, cur, nxt)
        return cur, nxt

    zero = jnp.zeros((nk, nl), F32)
    start = (
        tuple(jnp.where(low_south, zero, s[i]) for i in range(ni)),
        tuple(f[0, i] for i in range(ni)),
    )
    prev, cur = lax.fori_loop(0, rows - 1, body, start, unroll=False)
    row(rows - 1, prev, cur, tuple(jnp.where(low_south, s[i], zero) for i in range(ni)))


def full_body(flags, f, fj, fi, fk, ha, hb, e1, e2, s, order, out):
    _, ni, _, _ = f.shape

    def emit(j, new):
        for i in range(ni):
            out[j, i] = new[i]

    update_rows(flags, f, fj, fi, fk, ha, hb, e1, e2, s, emit)


def final_body(flags, f, fj, fi, fk, ha, hb, e1, e2, s, out, stats):
    rows, ni, nk, nl = f.shape

    def emit(j, new):
        for i in range(ni):
            out[j, i] = new[i]

    update_rows(flags, f, fj, fi, fk, ha, hb, e1, e2, s, emit)
    zero = tuple(jnp.zeros((nk, nl), F32) for _ in range(ni))

    def add(j, sums):
        return tuple(a + out[j, i] for i, a in enumerate(sums))

    means = tuple(a * (1.0 / rows) for a in lax.fori_loop(0, rows, add, zero, unroll=2))

    def add_square(j, sums):
        new = []
        for i, a in enumerate(sums):
            d = out[j, i] - means[i]
            new.append(a + d * d)
        return tuple(new)

    spread = lax.fori_loop(0, rows, add_square, zero, unroll=2)
    for i in range(ni):
        stats[0, i] = means[i]
        stats[1, i] = spread[i]


def scale_body(f, mine, other, out):
    rows, ni, _, _ = f.shape
    mean = []
    scale = []
    for i in range(ni):
        apart = mine[0, i] - other[0, i]
        mean.append(0.5 * (mine[0, i] + other[0, i]))
        squares = mine[1, i] + other[1, i] + (0.5 * rows) * (apart * apart)
        scale.append(lax.rsqrt(squares * (0.5 / rows) + 0.0001))

    def body(j, _):
        for i in range(ni):
            out[j, i] = (f[j, i] - mean[i]) * scale[i]
        return 0

    lax.fori_loop(0, rows, body, 0, unroll=2)


def first_a_body(flags, f, ga, sem):
    nk = f.shape[2]
    copy = pltpu.make_async_copy(f.at[:, :, jnp.where(flags[0] == 0, nk - 1, 0)], ga, sem)
    copy.start()
    copy.wait()


def first_rest_body(flags, f, order, gb, g1, g2, gs, sems):
    rows, ni, nk = f.shape[:3]
    i1 = jnp.where(flags[1] == 0, ni - 1, 0)
    copies = [
        pltpu.make_async_copy(src, dst, sems.at[n])
        for n, (src, dst) in enumerate(
            [
                (f.at[:, :, jnp.where(flags[0] == 0, 0, nk - 1)], gb),
                (f.at[:, ni - 1 - i1], g2),
                (f.at[:, i1], g1),
                (f.at[jnp.where(flags[2] == 0, rows - 1, 0)], gs),
            ]
        )
    ]
    for c in copies:
        c.start()
    for c in copies:
        c.wait()


def load_body(*refs):
    n = (len(refs) - 2) // 2
    copies = [
        pltpu.make_async_copy(refs[i], refs[n + 1 + i], refs[-1].at[i]) for i in range(n)
    ]
    for c in copies:
        c.start()
    for c in copies:
        c.wait()


def call(body, args, outs, mib=2, spaces=None, scratch=()):
    spaces = spaces or [VMEM] * len(args)
    if args[0].dtype == jnp.int32:
        spaces = [SMEM, *spaces[1:]]
    return pl.pallas_call(
        body,
        out_shape=[jax.ShapeDtypeStruct(o, F32) for o in outs],
        in_specs=[pl.BlockSpec(memory_space=m) for m in spaces],
        out_specs=[pl.BlockSpec(memory_space=VMEM) for _ in outs],
        scratch_shapes=scratch,
        compiler_params=pltpu.CompilerParams(vmem_limit_bytes=mib << 20),
    )(*args)


def per_device(field, fj, fi, fk):
    import functools

    rows, ni, nk, nl = field.shape
    flags = jnp.stack(
        [
            lax.axis_index("down") % 2,
            lax.axis_index("east") % 2,
            lax.axis_index("south"),
        ]
    ).astype(jnp.int32)

    def swap(x, axis, first):
        return lax.ppermute(x, axis, swap_pairs(lax.axis_size(axis), first))

    flat = (rows, ni * nk, nl)
    kface, iface, jface = (rows, ni, nl), (rows, nk, nl), (ni, nk, nl)
    sem = pltpu.SemaphoreType.DMA
    lines = field.reshape(rows, ni, nk, 1, nl)
    (ga,) = call(first_a_body, [flags, lines], [(rows, ni, 1, nl)], 51, [SMEM, HBM], [sem])
    ha = swap(ga.reshape(kface), "down", 0)
    gb, g1, g2, gs = call(
        first_rest_body, [flags, lines, ga],
        [(rows, ni, 1, nl), (rows, nk, 1, nl), (rows, nk, 1, nl), (ni, nk, 1, nl)],
        51, [SMEM, HBM, VMEM], [sem((4,))],
    )
    hb = swap(gb.reshape(kface), "down", 1)
    e2 = swap(g2.reshape(iface), "east", 1)
    s = swap(gs.reshape(jface), "south", 0)
    e1 = swap(g1.reshape(iface), "east", 0)
    field, fj, fi, fk = call(
        load_body, [field, fj, fi, fk, gs], [field.shape] * 4,
        32, [HBM] * 4 + [VMEM], [sem((4,))],
    )

    fjr, fir, fkr = (x.reshape(flat) for x in (fj, fi, fk))
    for _ in range(STEPS - 1):
        fr = field.reshape(flat)
        sr = s.reshape(ni * nk, nl)
        (ga,) = call(functools.partial(face_body, 0), [flags, fr, fjr, fir, fkr, ha, e1, e2, sr], [kface])
        ha_next = swap(ga, "down", 0)
        (gb,) = call(functools.partial(face_body, 1), [flags, fr, fjr, fir, fkr, hb, e1, e2, sr], [kface])
        hb_next = swap(gb, "down", 1)
        halos = [flags, field, fj, fi, fk, ha, hb, e1, e2, s]
        g1, g2, gs = call(edge_body, [*halos, gb], [iface, iface, jface])
        e2 = swap(g2, "east", 1)
        s = swap(gs, "south", 0)
        e1 = swap(g1, "east", 0)
        (field,) = call(full_body, [*halos, gs], [field.shape])
        ha, hb = ha_next, hb_next
    field, stats = call(
        final_body, [flags, field, fj, fi, fk, ha, hb, e1, e2, s],
        [field.shape, (2, ni, nk, nl)], 12,
    )
    other = swap(stats, "south", 0)
    (standardized,) = call(scale_body, [field, stats, other], [field.shape], 12)
    return (standardized, field)


def solution(mesh):
    spec = P("south", "east", "down", None)
    return jax.shard_map(
        per_device,
        mesh=mesh,
        in_specs=(spec,) * 4,
        out_specs=(spec, spec),
        check_vma=False,
    )
```

```python
import jax
import jax.numpy as jnp
from jax import lax
from jax.experimental import pallas as pl
from jax.experimental.pallas import tpu as pltpu
from jax.sharding import PartitionSpec as P


STEPS = 6
RATE = 0.05
F32 = jnp.float32
VMEM = pltpu.VMEM
SMEM = pltpu.SMEM
HBM = pltpu.HBM
ROWS = 8
QUAD = 4
PAIR = 2


def swap_pairs(devices, first):
    pairs = []
    for a in range(first, devices - 1, 2):
        pairs += [(a, a + 1), (a + 1, a)]
    return pairs


def combine(c, jl, ju, il, iu, kl, ku, fj, fi, fk):
    total = (jl + ju) + (il + iu) + (kl + ku)
    return (
        c * (1.0 - 6.0 * RATE)
        + RATE * total
        - fj * (ju - jl)
        - fi * (iu - il)
        - fk * (ku - kl)
    )


def face_body(side, flags, f, fj, fi, fk, halo, e1, e2, s, out):
    rows, ni, nl = out.shape
    nk = f.shape[1] // ni
    last = flags[0] == side
    k = jnp.where(last, nk - 1, 0)
    kin = jnp.where(last, nk - 2, 1)
    sign = jnp.where(last, F32(1), F32(-1))
    i_even = flags[1] == 0
    low_south = flags[2] == 0
    sub = lax.broadcasted_iota(jnp.int32, (ni, nl), 0)
    e1_edge = sub == jnp.where(i_even, ni - 1, 0)
    first_i = sub == 0
    last_i = sub == ni - 1

    def at(ref, j, kk):
        return ref[j, pl.ds(kk, ni, stride=nk), :]

    beyond = s[pl.ds(k, ni, stride=nk), :]
    zero = jnp.zeros_like(beyond)
    before = jnp.where(low_south, zero, beyond)
    after = jnp.where(low_south, beyond, zero)

    def body(t, prev):
        j0 = t * ROWS
        cur = [at(f, j0 + r, k) for r in range(ROWS)]
        nxt = jnp.where(j0 + ROWS == rows, after, at(f, jnp.minimum(j0 + ROWS, rows - 1), k))
        for r in range(ROWS):
            j, c = j0 + r, cur[r]
            r1 = jnp.broadcast_to(e1[j, pl.ds(k, 1), :], (ni, nl))
            r2 = jnp.broadcast_to(e2[j, pl.ds(k, 1), :], (ni, nl))
            edge = jnp.where(e1_edge, r1, r2)
            il = jnp.where(first_i, edge, pltpu.roll(c, 1, 0))
            iu = jnp.where(last_i, edge, pltpu.roll(c, ni - 1, 0))
            out[j] = combine(
                c, cur[r - 1] if r else prev, cur[r + 1] if r + 1 < ROWS else nxt,
                il, iu, at(f, j, kin), halo[j],
                at(fj, j, k), at(fi, j, k), sign * at(fk, j, k),
            )
        return cur[-1]

    lax.fori_loop(0, rows // ROWS, body, before)


def edge_body(flags, f, fj, fi, fk, ha, hb, e1, e2, s, order, g1, g2, gs):
    rows, ni, nk, nl = f.shape
    i_even = flags[1] == 0
    low_south = flags[2] == 0
    sub = lax.broadcasted_iota(jnp.int32, (nk, nl), 0)
    a_edge = sub == jnp.where(flags[0] == 0, nk - 1, 0)
    first_k = sub == 0
    last_k = sub == nk - 1
    zero = jnp.zeros((nk, nl), F32)

    def cell(j, i, c, prev, nxt, il, iu):
        ra = jnp.broadcast_to(ha[j, pl.ds(i, 1), :], (nk, nl))
        rb = jnp.broadcast_to(hb[j, pl.ds(i, 1), :], (nk, nl))
        edge = jnp.where(a_edge, ra, rb)
        kl = jnp.where(first_k, edge, pltpu.roll(c, 1, 0))
        ku = jnp.where(last_k, edge, pltpu.roll(c, nk - 1, 0))
        return combine(c, prev, nxt, il, iu, kl, ku, fj[j, i], fi[j, i], fk[j, i])

    def sides(j):
        x1, x2 = e1[j], e2[j]
        return jnp.where(i_even, x2, x1), jnp.where(i_even, x1, x2)

    js = jnp.where(low_south, rows - 1, 0)
    jin = jnp.where(low_south, rows - 2, 1)
    below, above = sides(js)
    row = [f[js, i] for i in range(ni)]
    for i in range(ni):
        inner = f[jin, i]
        gs[i] = cell(
            js, i, row[i], jnp.where(low_south, inner, s[i]), jnp.where(low_south, s[i], inner),
            row[i - 1] if i else below, row[i + 1] if i + 1 < ni else above,
        )

    before = tuple(jnp.where(low_south, zero, s[i]) for i in (0, ni - 1))
    after = tuple(jnp.where(low_south, s[i], zero) for i in (0, ni - 1))
    n = ROWS // 2

    def body(t, prev):
        j0 = t * n
        end = j0 + n == rows
        jn = jnp.minimum(j0 + n, rows - 1)
        cur = [(f[j0 + r, 0], f[j0 + r, ni - 1]) for r in range(n)]
        cur.append(tuple(jnp.where(end, a, f[jn, i]) for a, i in zip(after, (0, ni - 1))))
        cur.insert(0, prev)
        for r in range(n):
            j = j0 + r
            below, above = sides(j)
            lo = cell(j, 0, cur[r + 1][0], cur[r][0], cur[r + 2][0], below, f[j, 1])
            hi = cell(j, ni - 1, cur[r + 1][1], cur[r][1], cur[r + 2][1], f[j, ni - 2], above)
            g1[j] = jnp.where(i_even, hi, lo)
            g2[j] = jnp.where(i_even, lo, hi)
        return cur[n]

    lax.fori_loop(0, rows // n, body, before)


def sweep(flags, f, fj, fi, fk, ha, hb, e1, e2, s, start, visit, finish):
    rows, ni, nk, nl = f.shape
    i_even = flags[1] == 0
    low_south = flags[2] == 0
    sub = lax.broadcasted_iota(jnp.int32, (nk, nl), 0)
    a_edge = sub == jnp.where(flags[0] == 0, nk - 1, 0)
    first_k = sub == 0
    last_k = sub == nk - 1
    zero = jnp.zeros((nk, nl), F32)

    for i0 in range(0, ni, QUAD):
        quad = range(i0, i0 + QUAD)
        before = [jnp.where(low_south, zero, s[i]) for i in quad]
        after = [jnp.where(low_south, s[i], zero) for i in quad]

        def body(t, carry):
            prev, state = carry
            j0 = t * PAIR
            end = j0 + PAIR == rows
            jn = jnp.minimum(j0 + PAIR, rows - 1)
            cur = [prev]
            cur += [[f[j0 + r, i] for i in quad] for r in range(PAIR)]
            cur.append([jnp.where(end, a, f[jn, i]) for a, i in zip(after, quad)])
            for r in range(PAIR):
                j = j0 + r
                row = cur[r + 1]
                if i0 == 0:
                    below = jnp.where(i_even, e2[j], e1[j])
                else:
                    below = f[j, i0 - 1]
                if i0 + QUAD == ni:
                    above = jnp.where(i_even, e1[j], e2[j])
                else:
                    above = f[j, i0 + QUAD]
                line = [below, *row, above]
                new = []
                for n, i in enumerate(quad):
                    c = row[n]
                    ra = jnp.broadcast_to(ha[j, pl.ds(i, 1), :], (nk, nl))
                    rb = jnp.broadcast_to(hb[j, pl.ds(i, 1), :], (nk, nl))
                    edge = jnp.where(a_edge, ra, rb)
                    kl = jnp.where(first_k, edge, pltpu.roll(c, 1, 0))
                    ku = jnp.where(last_k, edge, pltpu.roll(c, nk - 1, 0))
                    new.append(
                        combine(
                            c, cur[r][n], cur[r + 2][n], line[n], line[n + 2], kl, ku,
                            fj[j, i], fi[j, i], fk[j, i],
                        )
                    )
                state = visit(j, r, quad, new, state)
            return cur[PAIR], state

        _, state = lax.fori_loop(0, rows // PAIR, body, (before, start(quad, zero)))
        finish(quad, state)


def full_body(flags, f, fj, fi, fk, ha, hb, e1, e2, s, order, out):
    def visit(j, r, quad, new, state):
        for i, x in zip(quad, new):
            out[j, i] = x
        return state

    sweep(
        flags, f, fj, fi, fk, ha, hb, e1, e2, s,
        lambda quad, zero: 0, visit, lambda quad, state: None,
    )


def final_body(flags, f, fj, fi, fk, ha, hb, e1, e2, s, out, stats):
    rows = f.shape[0]

    def start(quad, zero):
        return tuple([zero] * QUAD for _ in range(3))

    def visit(j, r, quad, new, state):
        shift, sums, squares = state
        if r == 0:
            shift = [jnp.where(j == 0, x, a) for x, a in zip(new, shift)]
        moved = [x - a for x, a in zip(new, shift)]
        for i, x in zip(quad, new):
            out[j, i] = x
        return (
            shift,
            [a + m for a, m in zip(sums, moved)],
            [a + m * m for a, m in zip(squares, moved)],
        )

    def finish(quad, state):
        for i, shift, total, square in zip(quad, *state):
            mean = total * (1.0 / rows)
            stats[0, i] = shift + mean
            stats[1, i] = jnp.maximum(square - total * mean, 0.0)

    sweep(flags, f, fj, fi, fk, ha, hb, e1, e2, s, start, visit, finish)


def scale_body(f, mine, other, out, buf, sems):
    rows, ni, _, _ = f.shape
    chunks = sems.shape[0]
    size = rows // chunks
    mean = []
    scale = []
    for i in range(ni):
        apart = mine[0, i] - other[0, i]
        mean.append(0.5 * (mine[0, i] + other[0, i]))
        squares = mine[1, i] + other[1, i] + (0.5 * rows) * (apart * apart)
        scale.append(lax.rsqrt(squares * (0.5 / rows) + 0.0001))

    def body(j, _):
        for i in range(ni):
            buf[j, i] = (f[j, i] - mean[i]) * scale[i]
        return 0

    copies = []
    for n in range(chunks):
        lax.fori_loop(n * size, (n + 1) * size, body, 0, unroll=2)
        part = pl.ds(n * size, size)
        copies.append(pltpu.make_async_copy(buf.at[part], out.at[part], sems.at[n]))
        copies[-1].start()
    for c in copies:
        c.wait()


def store_body(f, order, out, sem):
    copy = pltpu.make_async_copy(f, out, sem)
    copy.start()
    copy.wait()


def first_a_body(flags, f, ga, sem):
    nk = f.shape[2]
    copy = pltpu.make_async_copy(f.at[:, :, jnp.where(flags[0] == 0, nk - 1, 0)], ga, sem)
    copy.start()
    copy.wait()


def first_rest_body(flags, f, order, gb, g1, g2, gs, sems):
    rows, ni, nk = f.shape[:3]
    i1 = jnp.where(flags[1] == 0, ni - 1, 0)
    copies = [
        pltpu.make_async_copy(src, dst, sems.at[n])
        for n, (src, dst) in enumerate(
            [
                (f.at[:, :, jnp.where(flags[0] == 0, 0, nk - 1)], gb),
                (f.at[:, ni - 1 - i1], g2),
                (f.at[:, i1], g1),
                (f.at[jnp.where(flags[2] == 0, rows - 1, 0)], gs),
            ]
        )
    ]
    for c in copies:
        c.start()
    for c in copies:
        c.wait()


def load_body(*refs):
    n = (len(refs) - 2) // 2
    copies = [
        pltpu.make_async_copy(refs[i], refs[n + 1 + i], refs[-1].at[i]) for i in range(n)
    ]
    for c in copies:
        c.start()
    for c in copies:
        c.wait()


def call(body, args, outs, mib=2, spaces=None, scratch=(), out_space=VMEM):
    spaces = spaces or [VMEM] * len(args)
    if args[0].dtype == jnp.int32:
        spaces = [SMEM, *spaces[1:]]
    return pl.pallas_call(
        body,
        out_shape=[jax.ShapeDtypeStruct(o, F32) for o in outs],
        in_specs=[pl.BlockSpec(memory_space=m) for m in spaces],
        out_specs=[pl.BlockSpec(memory_space=out_space) for _ in outs],
        scratch_shapes=scratch,
        compiler_params=pltpu.CompilerParams(vmem_limit_bytes=mib << 20),
    )(*args)


def per_device(field, fj, fi, fk):
    import functools

    rows, ni, nk, nl = field.shape
    flags = jnp.stack(
        [
            lax.axis_index("down") % 2,
            lax.axis_index("east") % 2,
            lax.axis_index("south"),
        ]
    ).astype(jnp.int32)

    def swap(x, axis, first):
        return lax.ppermute(x, axis, swap_pairs(lax.axis_size(axis), first))

    flat = (rows, ni * nk, nl)
    kface, iface, jface = (rows, ni, nl), (rows, nk, nl), (ni, nk, nl)
    sem = pltpu.SemaphoreType.DMA
    lines = field.reshape(rows, ni, nk, 1, nl)
    (ga,) = call(first_a_body, [flags, lines], [(rows, ni, 1, nl)], 51, [SMEM, HBM], [sem])
    ha = swap(ga.reshape(kface), "down", 0)
    gb, g1, g2, gs = call(
        first_rest_body, [flags, lines, ga],
        [(rows, ni, 1, nl), (rows, nk, 1, nl), (rows, nk, 1, nl), (ni, nk, 1, nl)],
        51, [SMEM, HBM, VMEM], [sem((4,))],
    )
    hb = swap(gb.reshape(kface), "down", 1)
    e2 = swap(g2.reshape(iface), "east", 1)
    s = swap(gs.reshape(jface), "south", 0)
    e1 = swap(g1.reshape(iface), "east", 0)
    field, fj, fi, fk = call(
        load_body, [field, fj, fi, fk, gs], [field.shape] * 4,
        32, [HBM] * 4 + [VMEM], [sem((4,))],
    )

    fjr, fir, fkr = (x.reshape(flat) for x in (fj, fi, fk))
    for _ in range(STEPS - 1):
        fr = field.reshape(flat)
        sr = s.reshape(ni * nk, nl)
        (ga,) = call(functools.partial(face_body, 0), [flags, fr, fjr, fir, fkr, ha, e1, e2, sr], [kface])
        ha_next = swap(ga, "down", 0)
        (gb,) = call(functools.partial(face_body, 1), [flags, fr, fjr, fir, fkr, hb, e1, e2, sr], [kface])
        hb_next = swap(gb, "down", 1)
        halos = [flags, field, fj, fi, fk, ha, hb, e1, e2, s]
        g1, g2, gs = call(edge_body, [*halos, gb], [iface, iface, jface])
        e2 = swap(g2, "east", 1)
        s = swap(gs, "south", 0)
        e1 = swap(g1, "east", 0)
        (field,) = call(full_body, [*halos, gs], [field.shape])
        ha, hb = ha_next, hb_next
    field, stats = call(
        final_body, [flags, field, fj, fi, fk, ha, hb, e1, e2, s],
        [field.shape, (2, ni, nk, nl)],
    )
    other = swap(stats, "south", 0)
    (end,) = call(store_body, [field, stats], [field.shape], scratch=[sem], out_space=HBM)
    (standardized,) = call(
        scale_body, [field, stats, other], [field.shape], 8,
        scratch=[pltpu.VMEM(field.shape, F32), sem((8,))], out_space=HBM,
    )
    return (standardized, end)


def solution(mesh):
    spec = P("south", "east", "down", None)
    return jax.shard_map(
        per_device,
        mesh=mesh,
        in_specs=(spec,) * 4,
        out_specs=(spec, spec),
        check_vma=False,
    )
```

```python
import jax
import jax.numpy as jnp
from jax import lax
from jax.experimental import pallas as pl
from jax.experimental.pallas import tpu as pltpu
from jax.sharding import PartitionSpec as P


STEPS = 6
RATE = 0.05
F32 = jnp.float32
VMEM = pltpu.VMEM
SMEM = pltpu.SMEM
HBM = pltpu.HBM
ROWS = 8
QUAD = 4
PAIR = 2


def swap_pairs(devices, first):
    pairs = []
    for a in range(first, devices - 1, 2):
        pairs += [(a, a + 1), (a + 1, a)]
    return pairs


def combine(c, jl, ju, il, iu, kl, ku, fj, fi, fk):
    total = (jl + ju) + (il + iu) + (kl + ku)
    return (
        c * (1.0 - 6.0 * RATE)
        + RATE * total
        - fj * (ju - jl)
        - fi * (iu - il)
        - fk * (ku - kl)
    )


def face_body(side, flags, f, fj, fi, fk, halo, e1, e2, s, out):
    rows, ni, nl = out.shape
    nk = f.shape[1] // ni
    last = flags[0] == side
    k = jnp.where(last, nk - 1, 0)
    kin = jnp.where(last, nk - 2, 1)
    sign = jnp.where(last, F32(1), F32(-1))
    i_even = flags[1] == 0
    low_south = flags[2] == 0
    sub = lax.broadcasted_iota(jnp.int32, (ni, nl), 0)
    e1_edge = sub == jnp.where(i_even, ni - 1, 0)
    first_i = sub == 0
    last_i = sub == ni - 1

    def at(ref, j, kk):
        return ref[j, pl.ds(kk, ni, stride=nk), :]

    beyond = s[pl.ds(k, ni, stride=nk), :]
    zero = jnp.zeros_like(beyond)
    before = jnp.where(low_south, zero, beyond)
    after = jnp.where(low_south, beyond, zero)

    def body(t, prev):
        j0 = t * ROWS
        cur = [at(f, j0 + r, k) for r in range(ROWS)]
        nxt = jnp.where(j0 + ROWS == rows, after, at(f, jnp.minimum(j0 + ROWS, rows - 1), k))
        for r in range(ROWS):
            j, c = j0 + r, cur[r]
            r1 = jnp.broadcast_to(e1[j, pl.ds(k, 1), :], (ni, nl))
            r2 = jnp.broadcast_to(e2[j, pl.ds(k, 1), :], (ni, nl))
            edge = jnp.where(e1_edge, r1, r2)
            il = jnp.where(first_i, edge, pltpu.roll(c, 1, 0))
            iu = jnp.where(last_i, edge, pltpu.roll(c, ni - 1, 0))
            out[j] = combine(
                c, cur[r - 1] if r else prev, cur[r + 1] if r + 1 < ROWS else nxt,
                il, iu, at(f, j, kin), halo[j],
                at(fj, j, k), at(fi, j, k), sign * at(fk, j, k),
            )
        return cur[-1]

    lax.fori_loop(0, rows // ROWS, body, before)


def cells(flags, f, fj, fi, fk, ha, hb, e1, e2):
    _, _, nk, nl = f.shape
    i_even = flags[1] == 0
    sub = lax.broadcasted_iota(jnp.int32, (nk, nl), 0)
    a_edge = sub == jnp.where(flags[0] == 0, nk - 1, 0)
    first_k = sub == 0
    last_k = sub == nk - 1

    def cell(j, i, c, prev, nxt, il, iu):
        ra = jnp.broadcast_to(ha[j, pl.ds(i, 1), :], (nk, nl))
        rb = jnp.broadcast_to(hb[j, pl.ds(i, 1), :], (nk, nl))
        edge = jnp.where(a_edge, ra, rb)
        kl = jnp.where(first_k, edge, pltpu.roll(c, 1, 0))
        ku = jnp.where(last_k, edge, pltpu.roll(c, nk - 1, 0))
        return combine(c, prev, nxt, il, iu, kl, ku, fj[j, i], fi[j, i], fk[j, i])

    def sides(j):
        x1, x2 = e1[j], e2[j]
        return jnp.where(i_even, x2, x1), jnp.where(i_even, x1, x2)

    return cell, sides


def south_body(flags, f, fj, fi, fk, ha, hb, e1, e2, s, gs):
    rows, ni, _, _ = f.shape
    low_south = flags[2] == 0
    cell, sides = cells(flags, f, fj, fi, fk, ha, hb, e1, e2)
    js = jnp.where(low_south, rows - 1, 0)
    jin = jnp.where(low_south, rows - 2, 1)
    below, above = sides(js)
    row = [f[js, i] for i in range(ni)]
    for i in range(ni):
        inner = f[jin, i]
        gs[i] = cell(
            js, i, row[i], jnp.where(low_south, inner, s[i]), jnp.where(low_south, s[i], inner),
            row[i - 1] if i else below, row[i + 1] if i + 1 < ni else above,
        )


def face_b_body(flags, fr, fjr, fir, fkr, hb, e1, e2, sr, f, fj, fi, fk, ha, s, gb, gs):
    south_body(flags, f, fj, fi, fk, ha, hb, e1, e2, s, gs)
    face_body(1, flags, fr, fjr, fir, fkr, hb, e1, e2, sr, gb)


def edge_body(flags, f, fj, fi, fk, ha, hb, e1, e2, s, order, g1, g2):
    rows, ni, nk, nl = f.shape
    i_even = flags[1] == 0
    low_south = flags[2] == 0
    zero = jnp.zeros((nk, nl), F32)
    cell, sides = cells(flags, f, fj, fi, fk, ha, hb, e1, e2)

    before = tuple(jnp.where(low_south, zero, s[i]) for i in (0, ni - 1))
    after = tuple(jnp.where(low_south, s[i], zero) for i in (0, ni - 1))
    n = ROWS // 2

    def body(t, prev):
        j0 = t * n
        end = j0 + n == rows
        jn = jnp.minimum(j0 + n, rows - 1)
        cur = [(f[j0 + r, 0], f[j0 + r, ni - 1]) for r in range(n)]
        cur.append(tuple(jnp.where(end, a, f[jn, i]) for a, i in zip(after, (0, ni - 1))))
        cur.insert(0, prev)
        for r in range(n):
            j = j0 + r
            below, above = sides(j)
            lo = cell(j, 0, cur[r + 1][0], cur[r][0], cur[r + 2][0], below, f[j, 1])
            hi = cell(j, ni - 1, cur[r + 1][1], cur[r][1], cur[r + 2][1], f[j, ni - 2], above)
            g1[j] = jnp.where(i_even, hi, lo)
            g2[j] = jnp.where(i_even, lo, hi)
        return cur[n]

    lax.fori_loop(0, rows // n, body, before)


def sweep(flags, f, fj, fi, fk, ha, hb, e1, e2, s, start, visit, finish):
    rows, ni, nk, nl = f.shape
    i_even = flags[1] == 0
    low_south = flags[2] == 0
    sub = lax.broadcasted_iota(jnp.int32, (nk, nl), 0)
    a_edge = sub == jnp.where(flags[0] == 0, nk - 1, 0)
    first_k = sub == 0
    last_k = sub == nk - 1
    zero = jnp.zeros((nk, nl), F32)

    for i0 in range(0, ni, QUAD):
        quad = range(i0, i0 + QUAD)
        before = [jnp.where(low_south, zero, s[i]) for i in quad]
        after = [jnp.where(low_south, s[i], zero) for i in quad]

        def body(t, carry):
            prev, state = carry
            j0 = t * PAIR
            end = j0 + PAIR == rows
            jn = jnp.minimum(j0 + PAIR, rows - 1)
            cur = [prev]
            cur += [[f[j0 + r, i] for i in quad] for r in range(PAIR)]
            cur.append([jnp.where(end, a, f[jn, i]) for a, i in zip(after, quad)])
            for r in range(PAIR):
                j = j0 + r
                row = cur[r + 1]
                if i0 == 0:
                    below = jnp.where(i_even, e2[j], e1[j])
                else:
                    below = f[j, i0 - 1]
                if i0 + QUAD == ni:
                    above = jnp.where(i_even, e1[j], e2[j])
                else:
                    above = f[j, i0 + QUAD]
                line = [below, *row, above]
                new = []
                for n, i in enumerate(quad):
                    c = row[n]
                    ra = jnp.broadcast_to(ha[j, pl.ds(i, 1), :], (nk, nl))
                    rb = jnp.broadcast_to(hb[j, pl.ds(i, 1), :], (nk, nl))
                    edge = jnp.where(a_edge, ra, rb)
                    kl = jnp.where(first_k, edge, pltpu.roll(c, 1, 0))
                    ku = jnp.where(last_k, edge, pltpu.roll(c, nk - 1, 0))
                    new.append(
                        combine(
                            c, cur[r][n], cur[r + 2][n], line[n], line[n + 2], kl, ku,
                            fj[j, i], fi[j, i], fk[j, i],
                        )
                    )
                state = visit(j, r, quad, new, state)
            return cur[PAIR], state

        _, state = lax.fori_loop(0, rows // PAIR, body, (before, start(quad, zero)))
        finish(quad, state)


def full_body(flags, f, fj, fi, fk, ha, hb, e1, e2, s, order, out):
    def visit(j, r, quad, new, state):
        for i, x in zip(quad, new):
            out[j, i] = x
        return state

    sweep(
        flags, f, fj, fi, fk, ha, hb, e1, e2, s,
        lambda quad, zero: 0, visit, lambda quad, state: None,
    )


def final_body(flags, f, fj, fi, fk, ha, hb, e1, e2, s, out, stats):
    rows = f.shape[0]

    def start(quad, zero):
        return tuple([zero] * QUAD for _ in range(3))

    def visit(j, r, quad, new, state):
        shift, sums, squares = state
        if r == 0:
            shift = [jnp.where(j == 0, x, a) for x, a in zip(new, shift)]
        moved = [x - a for x, a in zip(new, shift)]
        for i, x in zip(quad, new):
            out[j, i] = x
        return (
            shift,
            [a + m for a, m in zip(sums, moved)],
            [a + m * m for a, m in zip(squares, moved)],
        )

    def finish(quad, state):
        for i, shift, total, square in zip(quad, *state):
            mean = total * (1.0 / rows)
            stats[0, i] = shift + mean
            stats[1, i] = jnp.maximum(square - total * mean, 0.0)

    sweep(flags, f, fj, fi, fk, ha, hb, e1, e2, s, start, visit, finish)


def scale_body(f, mine, other, out, buf, sems):
    rows, ni, _, _ = f.shape
    chunks = sems.shape[0]
    size = rows // chunks
    mean = []
    scale = []
    for i in range(ni):
        apart = mine[0, i] - other[0, i]
        mean.append(0.5 * (mine[0, i] + other[0, i]))
        squares = mine[1, i] + other[1, i] + (0.5 * rows) * (apart * apart)
        scale.append(lax.rsqrt(squares * (0.5 / rows) + 0.0001))

    def body(j, _):
        for i in range(ni):
            buf[j, i] = (f[j, i] - mean[i]) * scale[i]
        return 0

    copies = []
    for n in range(chunks):
        lax.fori_loop(n * size, (n + 1) * size, body, 0, unroll=2)
        part = pl.ds(n * size, size)
        copies.append(pltpu.make_async_copy(buf.at[part], out.at[part], sems.at[n]))
        copies[-1].start()
    for c in copies:
        c.wait()


def store_body(f, order, out, sem):
    copy = pltpu.make_async_copy(f, out, sem)
    copy.start()
    copy.wait()


def first_a_body(flags, f, ga, sem):
    nk = f.shape[2]
    copy = pltpu.make_async_copy(f.at[:, :, jnp.where(flags[0] == 0, nk - 1, 0)], ga, sem)
    copy.start()
    copy.wait()


def first_rest_body(flags, f, order, gb, g1, g2, gs, sems):
    rows, ni, nk = f.shape[:3]
    i1 = jnp.where(flags[1] == 0, ni - 1, 0)
    copies = [
        pltpu.make_async_copy(src, dst, sems.at[n])
        for n, (src, dst) in enumerate(
            [
                (f.at[:, :, jnp.where(flags[0] == 0, 0, nk - 1)], gb),
                (f.at[:, ni - 1 - i1], g2),
                (f.at[:, i1], g1),
                (f.at[jnp.where(flags[2] == 0, rows - 1, 0)], gs),
            ]
        )
    ]
    for c in copies:
        c.start()
    for c in copies:
        c.wait()


def load_body(*refs):
    n = (len(refs) - 2) // 2
    copies = [
        pltpu.make_async_copy(refs[i], refs[n + 1 + i], refs[-1].at[i]) for i in range(n)
    ]
    for c in copies:
        c.start()
    for c in copies:
        c.wait()


def call(body, args, outs, mib=2, spaces=None, scratch=(), out_space=VMEM):
    spaces = spaces or [VMEM] * len(args)
    if args[0].dtype == jnp.int32:
        spaces = [SMEM, *spaces[1:]]
    return pl.pallas_call(
        body,
        out_shape=[jax.ShapeDtypeStruct(o, F32) for o in outs],
        in_specs=[pl.BlockSpec(memory_space=m) for m in spaces],
        out_specs=[pl.BlockSpec(memory_space=out_space) for _ in outs],
        scratch_shapes=scratch,
        compiler_params=pltpu.CompilerParams(vmem_limit_bytes=mib << 20),
    )(*args)


def per_device(field, fj, fi, fk):
    import functools

    rows, ni, nk, nl = field.shape
    flags = jnp.stack(
        [
            lax.axis_index("down") % 2,
            lax.axis_index("east") % 2,
            lax.axis_index("south"),
        ]
    ).astype(jnp.int32)

    def swap(x, axis, first):
        return lax.ppermute(x, axis, swap_pairs(lax.axis_size(axis), first))

    flat = (rows, ni * nk, nl)
    kface, iface, jface = (rows, ni, nl), (rows, nk, nl), (ni, nk, nl)
    sem = pltpu.SemaphoreType.DMA
    lines = field.reshape(rows, ni, nk, 1, nl)
    (ga,) = call(first_a_body, [flags, lines], [(rows, ni, 1, nl)], 51, [SMEM, HBM], [sem])
    ha = swap(ga.reshape(kface), "down", 0)
    gb, g1, g2, gs = call(
        first_rest_body, [flags, lines, ga],
        [(rows, ni, 1, nl), (rows, nk, 1, nl), (rows, nk, 1, nl), (ni, nk, 1, nl)],
        51, [SMEM, HBM, VMEM], [sem((4,))],
    )
    s = swap(gs.reshape(jface), "south", 0)
    hb = swap(gb.reshape(kface), "down", 1)
    e2 = swap(g2.reshape(iface), "east", 1)
    e1 = swap(g1.reshape(iface), "east", 0)
    field, fj, fi, fk = call(
        load_body, [field, fj, fi, fk, gs], [field.shape] * 4,
        32, [HBM] * 4 + [VMEM], [sem((4,))],
    )

    fjr, fir, fkr = (x.reshape(flat) for x in (fj, fi, fk))
    for _ in range(STEPS - 1):
        fr = field.reshape(flat)
        sr = s.reshape(ni * nk, nl)
        (ga,) = call(functools.partial(face_body, 0), [flags, fr, fjr, fir, fkr, ha, e1, e2, sr], [kface])
        ha_next = swap(ga, "down", 0)
        halos = [flags, field, fj, fi, fk, ha, hb, e1, e2, s]
        gb, gs = call(
            face_b_body,
            [flags, fr, fjr, fir, fkr, hb, e1, e2, sr, field, fj, fi, fk, ha, s],
            [kface, jface],
        )
        s = swap(gs, "south", 0)
        hb_next = swap(gb, "down", 1)
        g1, g2 = call(edge_body, [*halos, gb], [iface, iface])
        e2 = swap(g2, "east", 1)
        e1 = swap(g1, "east", 0)
        (field,) = call(full_body, [*halos, g1], [field.shape])
        ha, hb = ha_next, hb_next
    field, stats = call(
        final_body, [flags, field, fj, fi, fk, ha, hb, e1, e2, s],
        [field.shape, (2, ni, nk, nl)],
    )
    other = swap(stats, "south", 0)
    (end,) = call(store_body, [field, stats], [field.shape], scratch=[sem], out_space=HBM)
    (standardized,) = call(
        scale_body, [field, stats, other], [field.shape], 8,
        scratch=[pltpu.VMEM(field.shape, F32), sem((8,))], out_space=HBM,
    )
    return (standardized, end)


def solution(mesh):
    spec = P("south", "east", "down", None)
    return jax.shard_map(
        per_device,
        mesh=mesh,
        in_specs=(spec,) * 4,
        out_specs=(spec, spec),
        check_vma=False,
    )
```
